32 devices in a mesh: seq: 8 (over z, y), ch: 4 (over x, core).
Axes of the slice: x: 2, y: 2, z: 4, core: 2. Of those that a mesh axis runs over, the one named last changes fastest.
Arguments:
- query_input: bfloat16 [1024, 2048], P('seq', 'ch'), may hold values from -6 to 6
- key_input: bfloat16 [1024, 2048], P('seq', 'ch'), may hold values from -6 to 6
- value_input: bfloat16 [1024, 2048], P('seq', 'ch'), may hold values from -6 to 6
- cotangent: bfloat16 [1024, 2048], P('seq', 'ch'), may hold values from -6 to 6
- filter_taps: float32 [1024, 2048], P('seq', 'ch'), may hold values from -0.1875 to 0.1875
- skip_gain: float32 [2048], P('ch'), may hold values from -2 to 2
Outputs:
- output: bfloat16 [1024, 2048], P('seq', 'ch')
- query_grad: bfloat16 [1024, 2048], P('seq', 'ch')
- key_grad: bfloat16 [1024, 2048], P('seq', 'ch')
- value_grad: bfloat16 [1024, 2048], P('seq', 'ch')
- filter_grad: float32 [1024, 2048], P('seq', 'ch')
- skip_grad: float32 [2048], P('ch')
- grad_rms: float32 [], replicated
The draws below stay inside these ranges and needn't reach their ends.
All inputs are finite; a program needn't handle non-finite values.
Results may differ from the reference program's by a relative error of at most 0.0014.
Values sent between devices are 32-bit elements; how exact they have to be, the bound alone decides.
A program may use at most 64 MiB of HBM per device.

```python
import math
import jax
import jax.numpy as jnp
from jax import lax

CH_DEV = 512
TOKENS = 1024
CHANNELS = 2048
N_CH = 4


def level_of(own_key, dims, cuts, least, top_value):
    loudness = 1.0
    for dim, parts in cuts:
        heights = jax.random.uniform(jax.random.fold_in(jax.random.fold_in(own_key, 6), dim), (parts,), jnp.float32, least / len(cuts), top_value / len(cuts))
        loudness = loudness * jnp.repeat(jnp.exp(heights), dims[dim] // parts).reshape((-1,) + (1,) * (len(dims) - 1 - dim))
    return loudness


def gaussian(key, dims, deviation, reach, pieces=(), held_as=jnp.bfloat16):
    entries = deviation * jax.random.normal(key, dims, jnp.float32)
    if pieces:
        entries = entries * level_of(key, dims, pieces, -0.22, 0.18)
    return jnp.clip(entries, -reach, reach).astype(held_as)


def setup_inputs(seed: int = 0) -> dict:
    splits = jax.random.split(jax.random.key(seed), 7)
    return {
        "query_input": gaussian(splits[0], (TOKENS, CHANNELS), 1.0, 6.0, ((0, 8), (1, 4))),
        "key_input": gaussian(splits[1], (TOKENS, CHANNELS), 1.0, 6.0, ((0, 8), (1, 4))),
        "value_input": gaussian(splits[2], (TOKENS, CHANNELS), 1.0, 6.0, ((0, 8), (1, 4))),
        "cotangent": gaussian(splits[3], (TOKENS, CHANNELS), 1.0, 6.0, ((0, 8), (1, 4))),
        "filter_taps": gaussian(splits[4], (TOKENS, CHANNELS), TOKENS ** -0.5, 0.1875, ((0, 8), (1, 4)), jnp.float32),
        "skip_gain": gaussian(splits[5], (CHANNELS,), 0.5, 2.0, ((0, 4),), jnp.float32),
    }


def one_group(operands):
    query_input, key_input, value_input, cotangent, filter_taps, skip_gain = operands
    query_val = query_input.astype(jnp.float32)
    key_val = key_input.astype(jnp.float32)
    value_val = value_input.astype(jnp.float32)
    cot_val = cotangent.astype(jnp.float32)
    mixed_in = key_val * value_val
    gated_cot = query_val * cot_val
    length = 2 * TOKENS
    mixed_spec = jnp.fft.rfft(mixed_in, n=length, axis=0)
    gated_spec = jnp.fft.rfft(gated_cot, n=length, axis=0)
    taps_spec = jnp.fft.rfft(filter_taps, n=length, axis=0)
    conv_out = jnp.fft.irfft(mixed_spec * taps_spec, n=length, axis=0)[:TOKENS]
    back_conv = jnp.fft.irfft(gated_spec * jnp.conj(taps_spec), n=length, axis=0)[:TOKENS]
    kernel_grad = jnp.fft.irfft(gated_spec * jnp.conj(mixed_spec), n=length, axis=0)[:TOKENS]
    inner_sum = conv_out + skip_gain[None, :] * mixed_in
    mixed_grad = back_conv + skip_gain[None, :] * gated_cot
    grad_scale = 1.0 / math.sqrt(TOKENS)
    return ((query_val * inner_sum).astype(jnp.bfloat16), (cot_val * inner_sum).astype(jnp.bfloat16), (mixed_grad * value_val).astype(jnp.bfloat16), (mixed_grad * key_val).astype(jnp.bfloat16), kernel_grad * grad_scale, lax.optimization_barrier(jnp.sum(gated_cot * mixed_in, axis=0)) * grad_scale)

def split_rows(array):
    return jnp.moveaxis(array.reshape(array.shape[0], N_CH, CH_DEV), 1, 0)

def join_rows(array):
    return jnp.moveaxis(array, 0, 1).reshape(array.shape[1], N_CH * CH_DEV)

def reference(query_input, key_input, value_input, cotangent, filter_taps, skip_gain):
    operands = (split_rows(query_input), split_rows(key_input), split_rows(value_input), split_rows(cotangent), split_rows(filter_taps), skip_gain.reshape(N_CH, CH_DEV))
    results = lax.map(one_group, operands)
    output = join_rows(results[0])
    query_grad = join_rows(results[1])
    key_grad = join_rows(results[2])
    value_grad = join_rows(results[3])
    filter_grad = join_rows(results[4])
    skip_grad = results[5].reshape(CHANNELS)
    squares = jnp.sum(filter_grad * filter_grad) + jnp.sum(skip_grad * skip_grad)
    grad_rms = jnp.sqrt(squares / (CHANNELS * (TOKENS + 1)))
    return (output, query_grad, key_grad, value_grad, filter_grad, skip_grad, grad_rms)
```

```python
import functools
import math

import jax
import jax.numpy as jnp
import numpy as np
from jax import lax
from jax.experimental import pallas as pl
from jax.experimental.pallas import tpu as pltpu
from jax.sharding import PartitionSpec as P

LANES = 128
MESH = pl.DeviceIdType.MESH


def complex_mul(left_op, right_op):
    return jnp.stack(
        [
            left_op[0] * right_op[0] - left_op[1] * right_op[1],
            left_op[0] * right_op[1] + left_op[1] * right_op[0],
        ]
    )


def conj_of(stacked):
    return jnp.stack([stacked[0], -stacked[1]])


def dft_table(length, direction):
    counter = jnp.arange(length)
    angles = (
        2.0 * math.pi / length * (counter[:, None] * counter[None, :] % length).astype(jnp.float32)
    )
    return (jnp.cos(angles), direction * jnp.sin(angles))


def dft_along(stacked, length, direction, pattern):
    table_re, table_im = dft_table(length, direction)

    def contract(table, part_in):
        return jnp.einsum(pattern, table, part_in, precision=lax.Precision.HIGHEST)

    real_out = contract(table_re, stacked[0]) - contract(table_im, stacked[1])
    imag_out = contract(table_re, stacked[1]) + contract(table_im, stacked[0])
    return jnp.stack([real_out, imag_out])


def grid_twiddle(devices, block, direction):
    seq_length = devices * block
    counter = jnp.arange(devices)[:, None] * jnp.arange(block)[None, :] % seq_length
    angles = direction * 2.0 * math.pi / seq_length * counter.astype(jnp.float32)
    return jnp.stack([jnp.cos(angles), jnp.sin(angles)])[:, None, None]


def local_forward(stacked, devices, block):
    array_shape = stacked.shape
    stacked = stacked.reshape(array_shape[0], array_shape[1], array_shape[2], devices, block)
    stacked = dft_along(stacked, devices, -1.0, "kj,scjp->sckp")
    stacked = complex_mul(stacked, grid_twiddle(devices, block, -1.0))
    return dft_along(stacked, block, -1.0, "kp,scjp->scjk")


def local_inverse(stacked, devices, block):
    stacked = dft_along(stacked, block, 1.0, "kp,scjp->scjk")
    stacked = complex_mul(stacked, grid_twiddle(devices, block, 1.0))
    stacked = dft_along(stacked, devices, 1.0, "kj,scjp->sckp")
    array_shape = stacked.shape
    return stacked.reshape(array_shape[0], array_shape[1], array_shape[2], devices * block) / (
        devices * block
    )


def modulated(signals, cosine, sine_part):
    zero_part = jnp.zeros_like(signals)
    return jnp.stack(
        [
            jnp.concatenate([signals, signals * cosine]),
            jnp.concatenate([zero_part, -signals * sine_part]),
        ]
    )


def spectral_products(spectrum):
    mixed_spec = spectrum[:, 0::3]
    gated_spec = spectrum[:, 1::3]
    taps_spec = spectrum[:, 2::3]
    out_spec = complex_mul(mixed_spec, taps_spec)
    back_spec = complex_mul(gated_spec, conj_of(taps_spec))
    grad_spec = complex_mul(gated_spec, conj_of(mixed_spec))
    return jnp.stack(
        [
            out_spec[:, 0],
            back_spec[:, 0],
            grad_spec[:, 0],
            out_spec[:, 1],
            back_spec[:, 1],
            grad_spec[:, 1],
        ],
        axis=1,
    )


def unfold(series, cosine, sine_part):
    return tuple(
        (
            0.5
            * (
                series[0, signal_index]
                + cosine * series[0, signal_index + 3]
                - sine_part * series[1, signal_index + 3]
            )
            for signal_index in range(3)
        )
    )


def channel_local(mixed_in, gated_cot, filter_taps, devices):
    pieces = (
        lax.all_to_all(mixed_in, "seq", split_axis=1, concat_axis=0, tiled=True),
        lax.all_to_all(gated_cot, "seq", split_axis=1, concat_axis=0, tiled=True),
        lax.all_to_all(filter_taps, "seq", split_axis=1, concat_axis=0, tiled=True),
    )
    laid = jnp.transpose(jnp.stack(pieces), (0, 2, 1))
    seq_length = laid.shape[2]
    block = seq_length // devices
    angles = math.pi / seq_length * jnp.arange(seq_length).astype(jnp.float32)
    cosine = jnp.cos(angles)
    sine_row = jnp.sin(angles)
    spectrum = local_forward(modulated(laid, cosine, sine_row), devices, block)
    series = local_inverse(spectral_products(spectrum), devices, block)
    results = unfold(series, cosine, sine_row)
    return (
        lax.all_to_all(results[0].T, "seq", split_axis=0, concat_axis=1, tiled=True),
        lax.all_to_all(results[1].T, "seq", split_axis=0, concat_axis=1, tiled=True),
        lax.all_to_all(results[2].T, "seq", split_axis=0, concat_axis=1, tiled=True),
    )


def body(query_input, key_input, value_input, cotangent, filter_taps, skip_gain):
    devices = lax.axis_size("seq")
    row_count, channels = query_input.shape
    seq_length = row_count * devices
    query_val = query_input.astype(jnp.float32)
    key_val = key_input.astype(jnp.float32)
    value_val = value_input.astype(jnp.float32)
    cot_val = cotangent.astype(jnp.float32)
    mixed_in = key_val * value_val
    gated_cot = query_val * cot_val
    conv_out, back_conv, kernel_grad = channel_local(mixed_in, gated_cot, filter_taps, devices)
    inner_sum = conv_out + skip_gain[None, :] * mixed_in
    mixed_grad = back_conv + skip_gain[None, :] * gated_cot
    output = (query_val * inner_sum).astype(jnp.bfloat16)
    query_grad = (cot_val * inner_sum).astype(jnp.bfloat16)
    key_grad = (mixed_grad * value_val).astype(jnp.bfloat16)
    value_grad = (mixed_grad * key_val).astype(jnp.bfloat16)
    time_scale = 1.0 / math.sqrt(seq_length)
    filter_grad = kernel_grad * time_scale
    filter_sq = jnp.sum(filter_grad * filter_grad)
    skip_part = jnp.sum(gated_cot * mixed_in, axis=0) * time_scale
    skip_grad = lax.psum(skip_part, "seq")
    total_sq = lax.psum(filter_sq + jnp.sum(skip_grad * skip_grad) / devices, ("seq", "ch"))
    grad_rms = jnp.sqrt(total_sq / (channels * lax.axis_size("ch") * (seq_length + 1)))
    return (output, query_grad, key_grad, value_grad, filter_grad, skip_grad, grad_rms)


def split_high_low(array):
    high = array.astype(jnp.bfloat16)
    return high, (array - high.astype(jnp.float32)).astype(jnp.bfloat16)


def half_tables(points):
    odd = 2 * np.arange(points, dtype=np.int64) + 1
    angles = math.pi / (4 * points) * (odd[:, None] * odd[None, :] % (8 * points))
    parts = []
    for table in (np.cos(angles), np.sin(angles)):
        table = table.astype(np.float32)
        high = table.astype(jnp.bfloat16)
        parts += [high, (table - high.astype(np.float32)).astype(jnp.bfloat16)]
    shift = math.pi / (4 * points) * odd[:, None] * np.ones((1, LANES))
    return np.stack(parts), np.stack([np.cos(shift), np.sin(shift)]).astype(np.float32)


def kernel(
    devices, groups, count,
    q_ref, k_ref, v_ref, c_ref, h_ref, skip_ref, table_hbm, twist_hbm,
    out_ref, dq_ref, dk_ref, dv_ref, dh_ref, dskip_ref, rms_ref,
    x_buf, g_buf, wide, send, recv, spec, prod, back, home, tail, tail_home, sq_send, sq_recv,
    table, twist, send_sem, recv_sem, own_sem, tail_send, tail_recv, sq_ssem, sq_rsem, load_sem,
):
    me = lax.axis_index("seq")
    mine = lax.axis_index("ch")
    rows, channels = q_ref.shape
    half = rows // 2
    points = half * devices
    low = LANES // 2
    time_scale = 1.0 / math.sqrt(2 * points)

    barrier = pltpu.get_barrier_semaphore()
    for k in range(1, devices):
        pl.semaphore_signal(
            barrier, inc=1, device_id={"seq": lax.rem(me + k, devices)}, device_id_type=MESH
        )
    for k in range(1, groups):
        pl.semaphore_signal(
            barrier, inc=1, device_id={"ch": lax.rem(mine + k, groups)}, device_id_type=MESH
        )
    loads = (
        pltpu.make_async_copy(table_hbm, table, load_sem.at[0]),
        pltpu.make_async_copy(twist_hbm, twist, load_sem.at[1]),
    )
    for load in loads:
        load.start()

    def remote(source, target, slot, k):
        peer = lax.rem(me + k, devices)
        return pltpu.make_async_remote_copy(
            src_ref=source.at[peer],
            dst_ref=target.at[me],
            send_sem=send_sem.at[slot, k],
            recv_sem=recv_sem.at[slot, k],
            device_id={"seq": peer},
            device_id_type=MESH,
        )

    def own(source, target, slot):
        return pltpu.make_async_copy(source.at[me], target.at[me], own_sem.at[slot])

    def tail_copy(k):
        peer = lax.rem(me + k, devices)
        return pltpu.make_async_remote_copy(
            src_ref=tail,
            dst_ref=tail_home.at[me],
            send_sem=tail_send.at[k],
            recv_sem=tail_recv.at[k],
            device_id={"seq": peer},
            device_id_type=MESH,
        )

    def square_copy(k):
        peer = lax.rem(mine + k, groups)
        return pltpu.make_async_remote_copy(
            src_ref=sq_send,
            dst_ref=sq_recv.at[mine],
            send_sem=sq_ssem.at[k],
            recv_sem=sq_rsem.at[k],
            device_id={"ch": peer},
            device_id_type=MESH,
        )

    def start_all(source, target, slot):
        for k in range(1, devices):
            remote(source, target, slot, k).start()
        own(source, target, slot).start()

    def wait_arrivals(source, target, slot):
        for k in range(1, devices):
            remote(source, target, slot, k).wait_recv()
        own(source, target, slot).wait()

    first = lax.broadcasted_iota(jnp.int32, (half, LANES), 1) < low

    def pack(source, signal):
        for j in range(channels // LANES):
            even = source[j, pl.ds(0, half, stride=2), :]
            odd = source[j, pl.ds(1, half, stride=2), :]
            send[signal, 2 * j] = jnp.where(first, even, pltpu.roll(odd, low, 1))
            send[signal, 2 * j + 1] = jnp.where(first, pltpu.roll(even, low, 1), odd)

    def unpack(signal):
        for j in range(channels // LANES):
            left = home[signal, 2 * j]
            right = home[signal, 2 * j + 1]
            wide[j, pl.ds(0, half, stride=2), :] = jnp.where(
                first, left, pltpu.roll(right, low, 1)
            )
            wide[j, pl.ds(1, half, stride=2), :] = jnp.where(
                first, pltpu.roll(left, low, 1), right
            )

    def columns_of(j):
        return pl.ds(j * LANES, LANES)

    blocks = channels // LANES
    for j in range(blocks):
        at = columns_of(j)
        x_buf[j] = k_ref[:, at].astype(jnp.float32) * v_ref[:, at].astype(jnp.float32)
    pack(x_buf, 0)
    pl.semaphore_wait(barrier, devices + groups - 2)
    start_all(send.at[0], recv.at[0], 0)
    for j in range(blocks):
        at = columns_of(j)
        g_buf[j] = q_ref[:, at].astype(jnp.float32) * c_ref[:, at].astype(jnp.float32)
    pack(g_buf, 1)
    start_all(send.at[1], recv.at[1], 1)
    for j in range(blocks):
        wide[j] = h_ref[:, columns_of(j)]
    pack(wide, 2)
    start_all(send.at[2], recv.at[2], 2)
    for load in loads:
        load.wait()

    def times(which, high, rest):
        both = jnp.concatenate([high, rest], axis=1)
        main = jnp.dot(table[2 * which], both, preferred_element_type=jnp.float32)
        small = jnp.dot(table[2 * which + 1], high, preferred_element_type=jnp.float32)
        return main[:, :LANES] + (main[:, LANES:] + small)

    def forward(signal):
        high, rest = split_high_low(recv[signal].reshape(points, LANES))
        spec[signal, 0] = times(0, high, rest)
        spec[signal, 1] = -times(1, high, rest)

    def inverse(slot, scale):
        real_high, real_rest = split_high_low(prod[0])
        imag_high, imag_rest = split_high_low(prod[1])
        series = times(0, real_high, real_rest) - times(1, imag_high, imag_rest)
        series = series * (scale / points)
        back[slot] = series.reshape(devices, half, LANES)
        return series

    step = 32

    def halves(ref_row, part, at):
        value = spec[ref_row, part, at, :]
        turned = pltpu.roll(value, low, 1)
        left = lax.broadcasted_iota(jnp.int32, (step, LANES), 1) < low
        return value, turned, jnp.where(left, value, turned), jnp.where(left, turned, value)

    def products(signal, other, conjugate):
        sign = jnp.where(lax.broadcasted_iota(jnp.int32, (step, LANES), 1) < low, 1.0, -1.0)

        @pl.loop(0, points // step)
        def _(index):
            at = pl.ds(pl.multiple_of(index * step, step), step)
            cosine = twist[0, at, :]
            sine = twist[1, at, :]
            signed = sine * sign
            _, _, even_re, odd_re = halves(other, 0, at)
            _, _, even_im, odd_im = halves(other, 1, at)
            a_re, as_re, _, _ = halves(signal, 0, at)
            a_im, as_im, _, _ = halves(signal, 1, at)
            p_re = even_re * cosine - even_im * sine
            p_im = even_im * cosine + even_re * sine
            if conjugate:
                r_re = odd_re * cosine - odd_im * signed
                r_im = odd_im * cosine + odd_re * signed
                prod[0, at, :] = a_re * p_re + a_im * p_im + (as_re * r_re + as_im * r_im)
                prod[1, at, :] = a_im * p_re - a_re * p_im + (as_im * r_re - as_re * r_im)
            else:
                r_re = odd_re * cosine + odd_im * signed
                r_im = odd_im * cosine - odd_re * signed
                prod[0, at, :] = a_re * p_re - a_im * p_im + (as_re * r_re - as_im * r_im)
                prod[1, at, :] = a_im * p_re + a_re * p_im + (as_im * r_re + as_re * r_im)

    wait_arrivals(send.at[0], recv.at[0], 0)
    forward(0)
    wait_arrivals(send.at[1], recv.at[1], 1)
    forward(1)
    products(1, 0, True)
    series = inverse(0, time_scale)
    start_all(back.at[0], home.at[0], 3)
    direct = jnp.sum(
        (recv[0] * recv[1]).reshape(points // 8, 8, LANES), axis=0
    )
    direct = jnp.sum(direct, axis=0, keepdims=True)
    direct = jnp.broadcast_to(direct, (8, LANES)) * time_scale
    direct = direct + pltpu.roll(direct, low, 1)
    squares = jnp.sum((series * series).reshape(points // 8, 8, LANES), axis=0)
    squares = squares + direct * direct * (1.0 / 16.0)
    sq_send[...] = squares
    for k in range(1, groups):
        square_copy(k).start()
    sq_own = pltpu.make_async_copy(sq_send, sq_recv.at[mine], load_sem.at[2])
    sq_own.start()

    wait_arrivals(send.at[2], recv.at[2], 2)
    forward(2)
    products(0, 2, False)
    inverse(1, 1.0)
    start_all(back.at[1], home.at[1], 4)
    for k in range(1, groups):
        square_copy(k).wait_recv()
    sq_own.wait()
    total = sq_recv[0]
    for k in range(1, groups):
        total = total + sq_recv[k]
    tail[0] = direct
    tail[1] = total
    for k in range(1, devices):
        tail_copy(k).start()
    tail_own = pltpu.make_async_copy(tail, tail_home.at[me], load_sem.at[3])
    tail_own.start()
    products(1, 2, True)
    inverse(2, 1.0)
    start_all(back.at[2], home.at[2], 5)

    wait_arrivals(back.at[0], home.at[0], 3)
    unpack(0)
    for j in range(blocks):
        dh_ref[:, columns_of(j)] = wide[j]

    wait_arrivals(back.at[1], home.at[1], 4)
    unpack(1)
    for j in range(blocks):
        at = columns_of(j)
        inner = wide[j] + skip_ref[:, at] * x_buf[j]
        out_ref[:, at] = (q_ref[:, at].astype(jnp.float32) * inner).astype(jnp.bfloat16)
        dq_ref[:, at] = (c_ref[:, at].astype(jnp.float32) * inner).astype(jnp.bfloat16)

    for k in range(1, devices):
        tail_copy(k).wait_recv()
    tail_own.wait()
    total = tail_home[0, 1]
    for k in range(1, devices):
        total = total + tail_home[k, 1]
    total = jnp.sum(jnp.sum(total, axis=0, keepdims=True), axis=1, keepdims=True)
    rms_ref[...] = jnp.sqrt(total / count)
    for j in range(blocks):
        left = lax.broadcasted_iota(jnp.int32, (8, LANES), 1) < low
        both = jnp.where(left, tail_home[2 * j, 0], tail_home[2 * j + 1, 0])
        dskip_ref[:, columns_of(j)] = both[0:1]

    wait_arrivals(back.at[2], home.at[2], 5)
    unpack(2)
    for j in range(blocks):
        at = columns_of(j)
        grad = wide[j] + skip_ref[:, at] * g_buf[j]
        dk_ref[:, at] = (v_ref[:, at].astype(jnp.float32) * grad).astype(jnp.bfloat16)
        dv_ref[:, at] = (k_ref[:, at].astype(jnp.float32) * grad).astype(jnp.bfloat16)

    for k in range(1, devices):
        for slot in range(3):
            remote(send.at[slot], recv.at[slot], slot, k).wait_send()
            remote(back.at[slot], home.at[slot], slot + 3, k).wait_send()
        tail_copy(k).wait_send()
    for k in range(1, groups):
        square_copy(k).wait_send()


def fused_body(query_input, key_input, value_input, cotangent, filter_taps, skip_gain):
    devices = lax.axis_size("seq")
    groups = lax.axis_size("ch")
    rows, channels = query_input.shape
    half = rows // 2
    points = half * devices
    tables, twists = half_tables(points)
    count = float(channels * groups * (rows * devices + 1))
    vmem = pl.BlockSpec(memory_space=pltpu.VMEM)
    hbm = pl.BlockSpec(memory_space=pl.ANY)
    narrow = jax.ShapeDtypeStruct((rows, channels), jnp.bfloat16)
    moved = (3, devices, half, LANES)
    results = pl.pallas_call(
        functools.partial(kernel, devices, groups, count),
        out_shape=(
            narrow,
            narrow,
            narrow,
            narrow,
            jax.ShapeDtypeStruct((rows, channels), jnp.float32),
            jax.ShapeDtypeStruct((1, channels), jnp.float32),
            jax.ShapeDtypeStruct((1, 1), jnp.float32),
        ),
        in_specs=[vmem] * 6 + [hbm] * 2,
        out_specs=(vmem,) * 7,
        scratch_shapes=[
            pltpu.VMEM((channels // LANES, rows, LANES), jnp.float32),
            pltpu.VMEM((channels // LANES, rows, LANES), jnp.float32),
            pltpu.VMEM((channels // LANES, rows, LANES), jnp.float32),
            pltpu.VMEM(moved, jnp.float32),
            pltpu.VMEM(moved, jnp.float32),
            pltpu.VMEM((3, 2, points, LANES), jnp.float32),
            pltpu.VMEM((2, points, LANES), jnp.float32),
            pltpu.VMEM(moved, jnp.float32),
            pltpu.VMEM(moved, jnp.float32),
            pltpu.VMEM((2, 8, LANES), jnp.float32),
            pltpu.VMEM((devices, 2, 8, LANES), jnp.float32),
            pltpu.VMEM((8, LANES), jnp.float32),
            pltpu.VMEM((groups, 8, LANES), jnp.float32),
            pltpu.VMEM(tables.shape, jnp.bfloat16),
            pltpu.VMEM(twists.shape, jnp.float32),
            pltpu.SemaphoreType.DMA((6, devices)),
            pltpu.SemaphoreType.DMA((6, devices)),
            pltpu.SemaphoreType.DMA((6,)),
            pltpu.SemaphoreType.DMA((devices,)),
            pltpu.SemaphoreType.DMA((devices,)),
            pltpu.SemaphoreType.DMA((groups,)),
            pltpu.SemaphoreType.DMA((groups,)),
            pltpu.SemaphoreType.DMA((4,)),
        ],
        compiler_params=pltpu.CompilerParams(collective_id=0, has_side_effects=True),
    )(
        query_input, key_input, value_input, cotangent, filter_taps,
        skip_gain.reshape(1, channels), jnp.asarray(tables), jnp.asarray(twists),
    )
    return (*results[:5], results[5].reshape(channels), results[6].reshape(()))


def pick_body(query_input, *others):
    devices = lax.axis_size("seq")
    rows, channels = query_input.shape
    fits = 2 * channels == LANES * devices and channels % LANES == 0 and rows % 16 == 0
    chosen = fused_body if fits and rows * devices <= 2048 else body
    return chosen(query_input, *others)


def solution(mesh):
    return jax.shard_map(
        pick_body,
        mesh=mesh,
        in_specs=(
            P("seq", "ch"),
            P("seq", "ch"),
            P("seq", "ch"),
            P("seq", "ch"),
            P("seq", "ch"),
            P("ch"),
        ),
        out_specs=(
            P("seq", "ch"),
            P("seq", "ch"),
            P("seq", "ch"),
            P("seq", "ch"),
            P("seq", "ch"),
            P("ch"),
            P(),
        ),
        check_vma=False,
    )
```

```python
import functools
import math

import jax
import jax.numpy as jnp
import numpy as np
from jax import lax
from jax.experimental import pallas as pl
from jax.experimental.pallas import tpu as pltpu
from jax.sharding import PartitionSpec as P

LANES = 128
MESH = pl.DeviceIdType.MESH


def complex_mul(left_op, right_op):
    return jnp.stack(
        [
            left_op[0] * right_op[0] - left_op[1] * right_op[1],
            left_op[0] * right_op[1] + left_op[1] * right_op[0],
        ]
    )


def conj_of(stacked):
    return jnp.stack([stacked[0], -stacked[1]])


def dft_table(length, direction):
    counter = jnp.arange(length)
    angles = (
        2.0 * math.pi / length * (counter[:, None] * counter[None, :] % length).astype(jnp.float32)
    )
    return (jnp.cos(angles), direction * jnp.sin(angles))


def dft_along(stacked, length, direction, pattern):
    table_re, table_im = dft_table(length, direction)

    def contract(table, part_in):
        return jnp.einsum(pattern, table, part_in, precision=lax.Precision.HIGHEST)

    real_out = contract(table_re, stacked[0]) - contract(table_im, stacked[1])
    imag_out = contract(table_re, stacked[1]) + contract(table_im, stacked[0])
    return jnp.stack([real_out, imag_out])


def grid_twiddle(devices, block, direction):
    seq_length = devices * block
    counter = jnp.arange(devices)[:, None] * jnp.arange(block)[None, :] % seq_length
    angles = direction * 2.0 * math.pi / seq_length * counter.astype(jnp.float32)
    return jnp.stack([jnp.cos(angles), jnp.sin(angles)])[:, None, None]


def local_forward(stacked, devices, block):
    array_shape = stacked.shape
    stacked = stacked.reshape(array_shape[0], array_shape[1], array_shape[2], devices, block)
    stacked = dft_along(stacked, devices, -1.0, "kj,scjp->sckp")
    stacked = complex_mul(stacked, grid_twiddle(devices, block, -1.0))
    return dft_along(stacked, block, -1.0, "kp,scjp->scjk")


def local_inverse(stacked, devices, block):
    stacked = dft_along(stacked, block, 1.0, "kp,scjp->scjk")
    stacked = complex_mul(stacked, grid_twiddle(devices, block, 1.0))
    stacked = dft_along(stacked, devices, 1.0, "kj,scjp->sckp")
    array_shape = stacked.shape
    return stacked.reshape(array_shape[0], array_shape[1], array_shape[2], devices * block) / (
        devices * block
    )


def modulated(signals, cosine, sine_part):
    zero_part = jnp.zeros_like(signals)
    return jnp.stack(
        [
            jnp.concatenate([signals, signals * cosine]),
            jnp.concatenate([zero_part, -signals * sine_part]),
        ]
    )


def spectral_products(spectrum):
    mixed_spec = spectrum[:, 0::3]
    gated_spec = spectrum[:, 1::3]
    taps_spec = spectrum[:, 2::3]
    out_spec = complex_mul(mixed_spec, taps_spec)
    back_spec = complex_mul(gated_spec, conj_of(taps_spec))
    grad_spec = complex_mul(gated_spec, conj_of(mixed_spec))
    return jnp.stack(
        [
            out_spec[:, 0],
            back_spec[:, 0],
            grad_spec[:, 0],
            out_spec[:, 1],
            back_spec[:, 1],
            grad_spec[:, 1],
        ],
        axis=1,
    )


def unfold(series, cosine, sine_part):
    return tuple(
        (
            0.5
            * (
                series[0, signal_index]
                + cosine * series[0, signal_index + 3]
                - sine_part * series[1, signal_index + 3]
            )
            for signal_index in range(3)
        )
    )


def channel_local(mixed_in, gated_cot, filter_taps, devices):
    pieces = (
        lax.all_to_all(mixed_in, "seq", split_axis=1, concat_axis=0, tiled=True),
        lax.all_to_all(gated_cot, "seq", split_axis=1, concat_axis=0, tiled=True),
        lax.all_to_all(filter_taps, "seq", split_axis=1, concat_axis=0, tiled=True),
    )
    laid = jnp.transpose(jnp.stack(pieces), (0, 2, 1))
    seq_length = laid.shape[2]
    block = seq_length // devices
    angles = math.pi / seq_length * jnp.arange(seq_length).astype(jnp.float32)
    cosine = jnp.cos(angles)
    sine_row = jnp.sin(angles)
    spectrum = local_forward(modulated(laid, cosine, sine_row), devices, block)
    series = local_inverse(spectral_products(spectrum), devices, block)
    results = unfold(series, cosine, sine_row)
    return (
        lax.all_to_all(results[0].T, "seq", split_axis=0, concat_axis=1, tiled=True),
        lax.all_to_all(results[1].T, "seq", split_axis=0, concat_axis=1, tiled=True),
        lax.all_to_all(results[2].T, "seq", split_axis=0, concat_axis=1, tiled=True),
    )


def body(query_input, key_input, value_input, cotangent, filter_taps, skip_gain):
    devices = lax.axis_size("seq")
    row_count, channels = query_input.shape
    seq_length = row_count * devices
    query_val = query_input.astype(jnp.float32)
    key_val = key_input.astype(jnp.float32)
    value_val = value_input.astype(jnp.float32)
    cot_val = cotangent.astype(jnp.float32)
    mixed_in = key_val * value_val
    gated_cot = query_val * cot_val
    conv_out, back_conv, kernel_grad = channel_local(mixed_in, gated_cot, filter_taps, devices)
    inner_sum = conv_out + skip_gain[None, :] * mixed_in
    mixed_grad = back_conv + skip_gain[None, :] * gated_cot
    output = (query_val * inner_sum).astype(jnp.bfloat16)
    query_grad = (cot_val * inner_sum).astype(jnp.bfloat16)
    key_grad = (mixed_grad * value_val).astype(jnp.bfloat16)
    value_grad = (mixed_grad * key_val).astype(jnp.bfloat16)
    time_scale = 1.0 / math.sqrt(seq_length)
    filter_grad = kernel_grad * time_scale
    filter_sq = jnp.sum(filter_grad * filter_grad)
    skip_part = jnp.sum(gated_cot * mixed_in, axis=0) * time_scale
    skip_grad = lax.psum(skip_part, "seq")
    total_sq = lax.psum(filter_sq + jnp.sum(skip_grad * skip_grad) / devices, ("seq", "ch"))
    grad_rms = jnp.sqrt(total_sq / (channels * lax.axis_size("ch") * (seq_length + 1)))
    return (output, query_grad, key_grad, value_grad, filter_grad, skip_grad, grad_rms)


def split_high_low(array):
    high = array.astype(jnp.bfloat16)
    return high, (array - high.astype(jnp.float32)).astype(jnp.bfloat16)


def half_tables(points):
    odd = 2 * np.arange(points, dtype=np.int64) + 1
    angles = math.pi / (4 * points) * (odd[:, None] * odd[None, :] % (8 * points))
    parts = []
    for table in (np.cos(angles), np.sin(angles)):
        table = table.astype(np.float32)
        high = table.astype(jnp.bfloat16)
        parts += [high, (table - high.astype(np.float32)).astype(jnp.bfloat16)]
    shift = math.pi / (4 * points) * odd[:, None] * np.ones((1, LANES))
    return np.stack(parts), np.stack([np.cos(shift), np.sin(shift)]).astype(np.float32)


def kernel(
    devices, groups, count,
    q_ref, k_ref, v_ref, c_ref, h_ref, table_hbm, twist_hbm,
    flat, dskip_ref, rms_ref,
    x_buf, g_buf, wide, send, recv, spec, prod, back, home, tail, tail_home, sq_send, sq_recv,
    table, twist, send_sem, recv_sem, own_sem, tail_send, tail_recv, sq_ssem, sq_rsem, load_sem,
):
    me = lax.axis_index("seq")
    mine = lax.axis_index("ch")
    rows, channels = q_ref.shape
    half = rows // 2
    points = half * devices
    low = LANES // 2
    time_scale = 1.0 / math.sqrt(2 * points)

    barrier = pltpu.get_barrier_semaphore()
    for k in range(1, devices):
        pl.semaphore_signal(
            barrier, inc=1, device_id={"seq": lax.rem(me + k, devices)}, device_id_type=MESH
        )
    for k in range(1, groups):
        pl.semaphore_signal(
            barrier, inc=1, device_id={"ch": lax.rem(mine + k, groups)}, device_id_type=MESH
        )
    loads = (
        pltpu.make_async_copy(table_hbm, table, load_sem.at[0]),
        pltpu.make_async_copy(twist_hbm, twist, load_sem.at[1]),
    )
    for load in loads:
        load.start()

    def remote(source, target, slot, k):
        peer = lax.rem(me + k, devices)
        return pltpu.make_async_remote_copy(
            src_ref=source.at[peer],
            dst_ref=target.at[me],
            send_sem=send_sem.at[slot, k],
            recv_sem=recv_sem.at[slot, k],
            device_id={"seq": peer},
            device_id_type=MESH,
        )

    def own(source, target, slot):
        return pltpu.make_async_copy(source.at[me], target.at[me], own_sem.at[slot])

    def tail_copy(k):
        peer = lax.rem(me + k, devices)
        return pltpu.make_async_remote_copy(
            src_ref=tail,
            dst_ref=tail_home.at[me],
            send_sem=tail_send.at[k],
            recv_sem=tail_recv.at[k],
            device_id={"seq": peer},
            device_id_type=MESH,
        )

    def square_copy(k):
        peer = lax.rem(mine + k, groups)
        return pltpu.make_async_remote_copy(
            src_ref=sq_send,
            dst_ref=sq_recv.at[mine],
            send_sem=sq_ssem.at[k],
            recv_sem=sq_rsem.at[k],
            device_id={"ch": peer},
            device_id_type=MESH,
        )

    def start_all(source, target, slot):
        for k in range(1, devices):
            remote(source, target, slot, k).start()
        own(source, target, slot).start()

    def wait_arrivals(source, target, slot):
        for k in range(1, devices):
            remote(source, target, slot, k).wait_recv()
        own(source, target, slot).wait()

    first = lax.broadcasted_iota(jnp.int32, (half, LANES), 1) < low

    def pack(source, signal):
        for j in range(channels // LANES):
            even = source[j, pl.ds(0, half, stride=2), :]
            odd = source[j, pl.ds(1, half, stride=2), :]
            send[signal, 2 * j] = jnp.where(first, even, pltpu.roll(odd, low, 1))
            send[signal, 2 * j + 1] = jnp.where(first, pltpu.roll(even, low, 1), odd)

    def unpack(signal):
        for j in range(channels // LANES):
            left = home[signal, 2 * j]
            right = home[signal, 2 * j + 1]
            flat[signal, j, pl.ds(0, half, stride=2), :] = jnp.where(
                first, left, pltpu.roll(right, low, 1)
            )
            flat[signal, j, pl.ds(1, half, stride=2), :] = jnp.where(
                first, pltpu.roll(left, low, 1), right
            )

    def columns_of(j):
        return pl.ds(j * LANES, LANES)

    blocks = channels // LANES
    for j in range(blocks):
        at = columns_of(j)
        x_buf[j] = k_ref[:, at].astype(jnp.float32) * v_ref[:, at].astype(jnp.float32)
    pack(x_buf, 0)
    pl.semaphore_wait(barrier, devices + groups - 2)
    start_all(send.at[0], recv.at[0], 0)
    for j in range(blocks):
        at = columns_of(j)
        g_buf[j] = q_ref[:, at].astype(jnp.float32) * c_ref[:, at].astype(jnp.float32)
    pack(g_buf, 1)
    start_all(send.at[1], recv.at[1], 1)
    for j in range(blocks):
        wide[j] = h_ref[:, columns_of(j)]
    pack(wide, 2)
    start_all(send.at[2], recv.at[2], 2)
    for load in loads:
        load.wait()

    def times(which, high, rest):
        both = jnp.concatenate([high, rest], axis=1)
        main = jnp.dot(table[2 * which], both, preferred_element_type=jnp.float32)
        small = jnp.dot(table[2 * which + 1], high, preferred_element_type=jnp.float32)
        return main[:, :LANES] + (main[:, LANES:] + small)

    def forward(signal):
        high, rest = split_high_low(recv[signal].reshape(points, LANES))
        spec[signal, 0] = times(0, high, rest)
        spec[signal, 1] = -times(1, high, rest)

    def inverse(slot, scale):
        real_high, real_rest = split_high_low(prod[0])
        imag_high, imag_rest = split_high_low(prod[1])
        series = times(0, real_high, real_rest) - times(1, imag_high, imag_rest)
        series = series * (scale / points)
        back[slot] = series.reshape(devices, half, LANES)
        return series

    step = 32

    def halves(ref_row, part, at):
        value = spec[ref_row, part, at, :]
        turned = pltpu.roll(value, low, 1)
        left = lax.broadcasted_iota(jnp.int32, (step, LANES), 1) < low
        return value, turned, jnp.where(left, value, turned), jnp.where(left, turned, value)

    def products(signal, other, conjugate):
        sign = jnp.where(lax.broadcasted_iota(jnp.int32, (step, LANES), 1) < low, 1.0, -1.0)

        @pl.loop(0, points // step)
        def _(index):
            at = pl.ds(pl.multiple_of(index * step, step), step)
            cosine = twist[0, at, :]
            sine = twist[1, at, :]
            signed = sine * sign
            _, _, even_re, odd_re = halves(other, 0, at)
            _, _, even_im, odd_im = halves(other, 1, at)
            a_re, as_re, _, _ = halves(signal, 0, at)
            a_im, as_im, _, _ = halves(signal, 1, at)
            p_re = even_re * cosine - even_im * sine
            p_im = even_im * cosine + even_re * sine
            if conjugate:
                r_re = odd_re * cosine - odd_im * signed
                r_im = odd_im * cosine + odd_re * signed
                prod[0, at, :] = a_re * p_re + a_im * p_im + (as_re * r_re + as_im * r_im)
                prod[1, at, :] = a_im * p_re - a_re * p_im + (as_im * r_re - as_re * r_im)
            else:
                r_re = odd_re * cosine + odd_im * signed
                r_im = odd_im * cosine - odd_re * signed
                prod[0, at, :] = a_re * p_re - a_im * p_im + (as_re * r_re - as_im * r_im)
                prod[1, at, :] = a_im * p_re + a_re * p_im + (as_im * r_re + as_re * r_im)

    wait_arrivals(send.at[0], recv.at[0], 0)
    forward(0)
    wait_arrivals(send.at[1], recv.at[1], 1)
    forward(1)
    products(1, 0, True)
    series = inverse(0, time_scale)
    start_all(back.at[0], home.at[0], 3)
    direct = jnp.sum(
        (recv[0] * recv[1]).reshape(points // 8, 8, LANES), axis=0
    )
    direct = jnp.sum(direct, axis=0, keepdims=True)
    direct = jnp.broadcast_to(direct, (8, LANES)) * time_scale
    direct = direct + pltpu.roll(direct, low, 1)
    squares = jnp.sum((series * series).reshape(points // 8, 8, LANES), axis=0)
    squares = squares + direct * direct * (1.0 / 16.0)
    sq_send[...] = squares
    for k in range(1, groups):
        square_copy(k).start()
    sq_own = pltpu.make_async_copy(sq_send, sq_recv.at[mine], load_sem.at[2])
    sq_own.start()

    wait_arrivals(send.at[2], recv.at[2], 2)
    forward(2)
    products(0, 2, False)
    inverse(1, 1.0)
    start_all(back.at[1], home.at[1], 4)
    for k in range(1, groups):
        square_copy(k).wait_recv()
    sq_own.wait()
    total = sq_recv[0]
    for k in range(1, groups):
        total = total + sq_recv[k]
    tail[0] = direct
    tail[1] = total
    for k in range(1, devices):
        tail_copy(k).start()
    tail_own = pltpu.make_async_copy(tail, tail_home.at[me], load_sem.at[3])
    tail_own.start()
    products(1, 2, True)
    inverse(2, 1.0)
    start_all(back.at[2], home.at[2], 5)

    wait_arrivals(back.at[0], home.at[0], 3)
    unpack(0)

    wait_arrivals(back.at[1], home.at[1], 4)
    unpack(1)

    for k in range(1, devices):
        tail_copy(k).wait_recv()
    tail_own.wait()
    total = tail_home[0, 1]
    for k in range(1, devices):
        total = total + tail_home[k, 1]
    total = jnp.sum(jnp.sum(total, axis=0, keepdims=True), axis=1, keepdims=True)
    rms_ref[...] = total / count
    for j in range(blocks):
        left = lax.broadcasted_iota(jnp.int32, (8, LANES), 1) < low
        both = jnp.where(left, tail_home[2 * j, 0], tail_home[2 * j + 1, 0])
        dskip_ref[:, columns_of(j)] = both[0:1]

    wait_arrivals(back.at[2], home.at[2], 5)
    unpack(2)

    for k in range(1, devices):
        for slot in range(3):
            remote(send.at[slot], recv.at[slot], slot, k).wait_send()
            remote(back.at[slot], home.at[slot], slot + 3, k).wait_send()
        tail_copy(k).wait_send()
    for k in range(1, groups):
        square_copy(k).wait_send()


def gate(
    q_ref, k_ref, v_ref, c_ref, skip_ref, flat, direct_ref, mean_ref,
    out_ref, dq_ref, dk_ref, dv_ref, dh_ref, dskip_ref, rms_ref,
):
    query_val = q_ref[...].astype(jnp.float32)
    key_val = k_ref[...].astype(jnp.float32)
    value_val = v_ref[...].astype(jnp.float32)
    cot_val = c_ref[...].astype(jnp.float32)
    skip = skip_ref[...]
    inner = flat[1, 0] + skip * (key_val * value_val)
    grad = flat[2, 0] + skip * (query_val * cot_val)
    out_ref[...] = (query_val * inner).astype(jnp.bfloat16)
    dq_ref[...] = (cot_val * inner).astype(jnp.bfloat16)
    dk_ref[...] = (grad * value_val).astype(jnp.bfloat16)
    dv_ref[...] = (grad * key_val).astype(jnp.bfloat16)
    dh_ref[...] = flat[0, 0]
    dskip_ref[...] = direct_ref[...]
    rms_ref[...] = jnp.sqrt(mean_ref[...])


def fused_body(query_input, key_input, value_input, cotangent, filter_taps, skip_gain):
    devices = lax.axis_size("seq")
    groups = lax.axis_size("ch")
    rows, channels = query_input.shape
    half = rows // 2
    points = half * devices
    tables, twists = half_tables(points)
    count = float(channels * groups * (rows * devices + 1))
    vmem = pl.BlockSpec(memory_space=pltpu.VMEM)
    hbm = pl.BlockSpec(memory_space=pl.ANY)
    narrow = jax.ShapeDtypeStruct((rows, channels), jnp.bfloat16)
    moved = (3, devices, half, LANES)
    blocks = channels // LANES
    flat, direct, rms = pl.pallas_call(
        functools.partial(kernel, devices, groups, count),
        out_shape=(
            jax.ShapeDtypeStruct((3, blocks, rows, LANES), jnp.float32),
            jax.ShapeDtypeStruct((1, channels), jnp.float32),
            jax.ShapeDtypeStruct((1, 1), jnp.float32),
        ),
        in_specs=[vmem] * 5 + [hbm] * 2,
        out_specs=(vmem,) * 3,
        scratch_shapes=[
            pltpu.VMEM((channels // LANES, rows, LANES), jnp.float32),
            pltpu.VMEM((channels // LANES, rows, LANES), jnp.float32),
            pltpu.VMEM((channels // LANES, rows, LANES), jnp.float32),
            pltpu.VMEM(moved, jnp.float32),
            pltpu.VMEM(moved, jnp.float32),
            pltpu.VMEM((3, 2, points, LANES), jnp.float32),
            pltpu.VMEM((2, points, LANES), jnp.float32),
            pltpu.VMEM(moved, jnp.float32),
            pltpu.VMEM(moved, jnp.float32),
            pltpu.VMEM((2, 8, LANES), jnp.float32),
            pltpu.VMEM((devices, 2, 8, LANES), jnp.float32),
            pltpu.VMEM((8, LANES), jnp.float32),
            pltpu.VMEM((groups, 8, LANES), jnp.float32),
            pltpu.VMEM(tables.shape, jnp.bfloat16),
            pltpu.VMEM(twists.shape, jnp.float32),
            pltpu.SemaphoreType.DMA((6, devices)),
            pltpu.SemaphoreType.DMA((6, devices)),
            pltpu.SemaphoreType.DMA((6,)),
            pltpu.SemaphoreType.DMA((devices,)),
            pltpu.SemaphoreType.DMA((devices,)),
            pltpu.SemaphoreType.DMA((groups,)),
            pltpu.SemaphoreType.DMA((groups,)),
            pltpu.SemaphoreType.DMA((4,)),
        ],
        compiler_params=pltpu.CompilerParams(collective_id=0, has_side_effects=True),
    )(
        query_input, key_input, value_input, cotangent, filter_taps, jnp.asarray(tables), jnp.asarray(twists),
    )
    column = pl.BlockSpec((rows, LANES), lambda j: (0, j))
    line = pl.BlockSpec((1, LANES), lambda j: (0, j))
    single = pl.BlockSpec((1, 1), lambda j: (0, 0))
    results = pl.pallas_call(
        gate,
        grid=(blocks,),
        out_shape=(
            narrow,
            narrow,
            narrow,
            narrow,
            jax.ShapeDtypeStruct((rows, channels), jnp.float32),
            jax.ShapeDtypeStruct((1, channels), jnp.float32),
            jax.ShapeDtypeStruct((1, 1), jnp.float32),
        ),
        in_specs=[column] * 4
        + [line, pl.BlockSpec((3, 1, rows, LANES), lambda j: (0, j, 0, 0)), line, single],
        out_specs=[column] * 5 + [line, single],
    )(
        query_input, key_input, value_input, cotangent,
        skip_gain.reshape(1, channels), flat, direct, rms,
    )
    return (*results[:5], results[5].reshape(channels), results[6].reshape(()))


def pick_body(query_input, *others):
    devices = lax.axis_size("seq")
    rows, channels = query_input.shape
    fits = 2 * channels == LANES * devices and channels % LANES == 0 and rows % 16 == 0
    chosen = fused_body if fits and rows * devices <= 2048 else body
    return chosen(query_input, *others)


def solution(mesh):
    return jax.shard_map(
        pick_body,
        mesh=mesh,
        in_specs=(
            P("seq", "ch"),
            P("seq", "ch"),
            P("seq", "ch"),
            P("seq", "ch"),
            P("seq", "ch"),
            P("ch"),
        ),
        out_specs=(
            P("seq", "ch"),
            P("seq", "ch"),
            P("seq", "ch"),
            P("seq", "ch"),
            P("seq", "ch"),
            P("ch"),
            P(),
        ),
        check_vma=False,
    )
```
